32 devices in a mesh: tm: 4 (over y, x), sat: 8 (over z, core).
Axes of the slice: x: 2, y: 2, z: 4, core: 2. Of those that a mesh axis runs over, the one named last changes fastest.
Arguments:
- samples: int32 [2, 8, 8192], P(None, 'tm', 'sat'), may hold values from -1073741824 to 1073741823
- codes: int32 [24, 4092], P('sat'), may hold values from -1 to 1, as said below
- dopplers: int32 [16], replicated, may hold values from -60 to 60
Outputs:
- power: float32 [16, 24, 8192], P('tm', 'sat')
- detection: float32 [24], P('sat')
The draws below stay inside these ranges and needn't reach their ends.
Inputs may be any that keep to these rules, and one draw needn't show every extreme that they name: `codes`: each entry is -1 or 1.
All inputs are finite; a program needn't handle non-finite values.
Results may differ from the reference program's by a relative error of at most 0.0003.
Values sent between devices are 32-bit elements.
A program may use at most 64 MiB of HBM per device.

```python
import math
import jax
import jax.numpy as jnp
from jax import lax

N = 8192
CHIPS = 4092
BLOCK_COUNT = 8
DOPPLER = 16
SATS = 24


def draw_samples(key, part):
    key_raw = jax.random.fold_in(key, 11)
    key_shift = jax.random.fold_in(key, 12)
    raw_words = jax.random.randint(key_raw, (2, BLOCK_COUNT, N), -1073741824, 1073741824, dtype=jnp.int32)
    shifts = jax.random.randint(key_shift, (2, BLOCK_COUNT, 32), 0, 3, dtype=jnp.int32)
    shifts = jnp.repeat(shifts, N // 32, axis=2)
    return jnp.right_shift(raw_words, shifts)


def draw_codes(key, part):
    chip_bits = jax.random.randint(jax.random.fold_in(key, 21), (SATS, CHIPS), 0, 2, dtype=jnp.int32)
    return 2 * chip_bits - 1


def with_ends(entries, stream_key, smallest, top_value):
    spot = [jax.random.randint(jax.random.fold_in(stream_key, axis), (), 0, length) for axis, length in enumerate(entries.shape)]
    main_axis = entries.shape.index(max(entries.shape))
    neighbour = spot[:main_axis] + [(spot[main_axis] + 1) % entries.shape[main_axis]] + spot[main_axis + 1:]
    return entries.at[tuple(spot)].set(smallest).at[tuple(neighbour)].set(top_value)


def setup_inputs(seed: int = 0) -> dict:
    seeds = jax.random.split(jax.random.key(seed), 4)
    return {
        "samples": draw_samples(jax.random.fold_in(seeds[3], 71), 0),
        "codes": draw_codes(jax.random.fold_in(seeds[3], 71), 0),
        "dopplers": with_ends(jax.random.randint(seeds[2], (DOPPLER,), -60, 61), jax.random.fold_in(seeds[2], 1), -60, 60).astype(jnp.int32),
    }


sample_scale = 2.0 ** -29
wrap_count = 32768


def replica_rows(codes):
    offsets = jnp.arange(N, dtype=jnp.int32)
    chip_index = (offsets * CHIPS) // N
    halves = jnp.mod((offsets * (2 * CHIPS)) // N, 2)
    sign_rows = (1 - 2 * halves).astype(jnp.float32)
    return jnp.take(codes, chip_index, axis=1).astype(jnp.float32) * sign_rows[None, :]


def reference(samples, codes, dopplers):
    real_part = samples[0].astype(jnp.float32) * sample_scale
    imag_part = samples[1].astype(jnp.float32) * sample_scale
    received_record = lax.complex(real_part, imag_part)
    spectrum = jnp.conj(jnp.fft.fft(replica_rows(codes), axis=-1))
    offsets = jnp.arange(N, dtype=jnp.int32)

    def one_bin(doppler_bin):
        rotation_angles = jnp.mod(doppler_bin * offsets, wrap_count).astype(jnp.float32) * (2.0 * math.pi / wrap_count)
        doppler_mixer = lax.complex(jnp.cos(rotation_angles), -jnp.sin(rotation_angles))
        wiped_record = jnp.fft.fft(received_record * doppler_mixer[None, :], axis=-1)

        def one_sat(code_spec):
            lagged = jnp.fft.ifft(wiped_record * code_spec[None, :], axis=-1)
            return jnp.sum(jnp.real(lagged) ** 2 + jnp.imag(lagged) ** 2, axis=0)

        return lax.map(one_sat, spectrum)

    power_map = lax.map(one_bin, dopplers) * (1.0 / (N * BLOCK_COUNT))
    average_energy = jnp.sum(real_part * real_part + imag_part * imag_part) / (BLOCK_COUNT * N)
    peak_value = jnp.max(power_map, axis=(0, 2))
    detection = peak_value / jnp.maximum(average_energy, 0.25)
    return (power_map, detection)
```

```python
import functools
import math

import jax
import jax.numpy as jnp
import ml_dtypes
import numpy as np
from jax import lax
from jax.experimental import pallas as pl
from jax.experimental.pallas import tpu as pltpu
from jax.sharding import PartitionSpec as P

sample_scale = 2.0 ** (-29)
wrap_count = 32768
LANES = 128


def halves(table):
    high = table.astype(np.float32).astype(ml_dtypes.bfloat16)
    low = (table - high.astype(np.float64)).astype(np.float32).astype(ml_dtypes.bfloat16)
    return high, low


@functools.lru_cache(maxsize=None)
def tables(sample_length, chip_count):
    inner = LANES
    outer = sample_length // inner
    a = np.arange(outer)
    c = np.arange(inner)
    ang_o = 2 * np.pi * (np.outer(a, a) % outer) / outer
    ang_t = 2 * np.pi * (np.outer(a, c) % sample_length) / sample_length
    ang_i = 2 * np.pi * (np.outer(c, c) % inner) / inner
    fc, fs = np.cos(ang_o), -np.sin(ang_o)
    first = np.block([[fc, -fs], [fs, fc]])
    second = np.block([[-fs, -fc], [fc, -fs]])
    wc, ws = np.cos(ang_i), -np.sin(ang_i)
    fh, fl = halves(np.block([[wc, ws], [-ws, wc]]))
    ih, il = halves(np.block([[wc, -ws], [ws, wc]]))
    bh, bl = halves(np.block([[fc, fs], [-fs, fc]]))
    ch, cl = halves(np.concatenate([fc, fs], axis=0))
    offsets = np.arange(sample_length).reshape(outer, inner)
    chips = offsets * chip_count // sample_length
    signs = 1 - 2 * ((offsets * 2 * chip_count // sample_length) % 2)
    starts = tuple(int(v) for v in chips[:, 0])
    within = chips - chips[:, :1]
    return dict(
        first=first.astype(np.float32),
        second=second.astype(np.float32),
        twist=np.stack([np.cos(ang_t), -np.sin(ang_t)]).astype(np.float32),
        fwd=np.concatenate([fh, fh, fl], axis=0),
        inv=np.concatenate([ih, ih, il], axis=0),
        back=np.concatenate([bh, bh, bl], axis=1),
        code=np.concatenate([ch, cl], axis=1),
        within=within.astype(np.int32),
        signs=signs.astype(np.float32),
    ), starts


NAMES = ("first", "second", "twist", "fwd", "inv", "back", "code", "within", "signs")


def split(value):
    high = value.astype(jnp.bfloat16)
    low = (value - high.astype(jnp.float32)).astype(jnp.bfloat16)
    return high, low


def mm(left, right):
    return jnp.dot(left, right, preferred_element_type=jnp.float32)


def kernel(starts, outer, chip_count, x_ref, codes_ref, dop_ref, first_ref, second_ref, twist_ref,
           fwd_ref, inv_ref, back_ref, code_ref, within_ref, signs_ref,
           power_ref, peak_ref, cpad, gath, cspec, rot, dtw, energy):
    inner = LANES
    tm_count, sat_count, _, own, rows, _ = x_ref.shape
    blocks = tm_count * own
    dop_rows, sats = power_ref.shape[0], power_ref.shape[1]
    sample_length = outer * inner

    cpad[...] = jnp.zeros_like(cpad)
    cpad[0:sats, 0:chip_count] = codes_ref[...].astype(jnp.float32)
    for n1 in range(outer):
        base = starts[n1] // LANES * LANES
        shift = starts[n1] - base
        piece = cpad[:, base:base + 2 * LANES]
        if shift:
            piece = pltpu.roll(piece, 2 * LANES - shift, 1)
        for s in range(sats):
            gath[s, n1:n1 + 1, :] = piece[s:s + 1, :LANES]
    scale = math.sqrt(1.0 / (float(sample_length) ** 3 * blocks))
    t_re, t_im = twist_ref[0], twist_ref[1]
    for s in range(sats):
        rep = jnp.take_along_axis(gath[s], within_ref[...], axis=1) * signs_ref[...]
        rep = rep.astype(jnp.bfloat16)
        y = mm(code_ref[...], jnp.concatenate([rep, rep], axis=0))
        y_re, y_im = y[:outer], y[outer:]
        z = jnp.concatenate([y_re * t_re - y_im * t_im, y_re * t_im + y_im * t_re], axis=1)
        zh, zl = split(z)
        cspec[s] = mm(jnp.concatenate([zh, zl, zh], axis=1), fwd_ref[...]) * scale

    col = lax.broadcasted_iota(jnp.int32, (8, inner), 1)
    row_of = lax.rem(col, outer) * inner
    base_row = lax.axis_index("tm") * dop_rows
    for f in range(dop_rows):
        d = dop_ref[base_row + f]
        turn = 2.0 * math.pi / wrap_count
        a1 = ((row_of * d) & (wrap_count - 1)).astype(jnp.float32) * turn
        a2 = ((col * d) & (wrap_count - 1)).astype(jnp.float32) * turn
        c1, s1 = jnp.cos(a1)[0:1], -jnp.sin(a1)[0:1]
        c2, s2 = jnp.cos(a2)[0:1], -jnp.sin(a2)[0:1]
        mh, ml = split(first_ref[...] * c1 + second_ref[...] * s1)
        rot[f] = jnp.concatenate([mh, mh, ml], axis=1)
        dtw[f, 0] = t_re * c2 - t_im * s2
        dtw[f, 1] = t_re * s2 + t_im * c2

    energy[...] = jnp.zeros_like(energy)
    power_ref[...] = jnp.zeros_like(power_ref)

    def pair(g, carry):
        cols = []
        for blk in range(own):
            parts = [x_ref[g, q, part, blk] for part in range(2) for q in range(sat_count)]
            cols.append(jnp.concatenate(parts, axis=0))
        x = jnp.concatenate(cols, axis=1).astype(jnp.float32) * sample_scale
        sq = x * x
        energy[...] += jnp.sum(sq.reshape(2 * outer // 8, 8, own * inner), axis=0)
        xh, xl = split(x)
        xs = jnp.concatenate([xh, xl, xh], axis=0)
        for f in range(dop_rows):
            y = mm(rot[f], xs)
            u_re, u_im = dtw[f, 0], dtw[f, 1]
            zs = []
            for blk in range(own):
                y_re = y[:outer, blk * inner:(blk + 1) * inner]
                y_im = y[outer:, blk * inner:(blk + 1) * inner]
                zs.append(jnp.concatenate([y_re * u_re - y_im * u_im, y_re * u_im + y_im * u_re], axis=1))
            zh, zl = split(jnp.concatenate(zs, axis=0))
            spec = mm(jnp.concatenate([zh, zl, zh], axis=1), fwd_ref[...])
            crosses = []
            for s in range(sats):
                k_re, k_im = cspec[s, :, :inner], cspec[s, :, inner:]
                for blk in range(own):
                    s_re = spec[blk * outer:(blk + 1) * outer, :inner]
                    s_im = spec[blk * outer:(blk + 1) * outer, inner:]
                    crosses.append(jnp.concatenate(
                        [s_re * k_re + s_im * k_im, s_im * k_re - s_re * k_im], axis=1))
            ch, cl = split(jnp.concatenate(crosses, axis=0))
            lag = mm(jnp.concatenate([ch, cl, ch], axis=1), inv_ref[...])
            for s in range(sats):
                cols = []
                for blk in range(own):
                    at = (s * own + blk) * outer
                    l_re, l_im = lag[at:at + outer, :inner], lag[at:at + outer, inner:]
                    cols.append(jnp.concatenate(
                        [l_re * t_re + l_im * t_im, l_im * t_re - l_re * t_im], axis=0))
                wh, wl = split(jnp.concatenate(cols, axis=1))
                out = mm(back_ref[...], jnp.concatenate([wh, wl, wh], axis=0))
                o_re, o_im = out[:outer], out[outer:]
                p = o_re * o_re + o_im * o_im
                total = p[:, :inner]
                for blk in range(1, own):
                    total = total + p[:, blk * inner:(blk + 1) * inner]
                power_ref[f, s] += total
        return carry

    lax.fori_loop(0, tm_count, pair, 0)
    mean = jnp.sum(energy[...]) * (1.0 / float(blocks * sample_length))
    floor = jnp.maximum(mean, 0.25)
    for s in range(sats):
        top = power_ref[0, s]
        for f in range(1, dop_rows):
            top = jnp.maximum(top, power_ref[f, s])
        peak_ref[s:s + 1, :] = jnp.full((1, LANES), jnp.max(top), jnp.float32) / floor


def shards(samples, codes, dopplers):
    tm_count, sat_count = lax.axis_size("tm"), lax.axis_size("sat")
    own, segment = samples.shape[1], samples.shape[2]
    sample_length = segment * sat_count
    outer, rows = sample_length // LANES, segment // LANES
    sats, chip_count = codes.shape
    dop_rows = dopplers.shape[0] // tm_count
    consts, starts = tables(sample_length, chip_count)
    local = samples.reshape(2, own, rows, LANES)
    whole = lax.all_gather(local, ("tm", "sat"), axis=0)
    whole = whole.reshape(tm_count, sat_count, 2, own, rows, LANES)
    pad = (max(starts) // LANES + 2) * LANES
    pad = max(pad, -(-chip_count // LANES) * LANES)
    vm = pl.BlockSpec(memory_space=pltpu.VMEM)
    power, peak = pl.pallas_call(
        functools.partial(kernel, starts, outer, chip_count),
        out_shape=(
            jax.ShapeDtypeStruct((dop_rows, sats, outer, LANES), jnp.float32),
            jax.ShapeDtypeStruct((sats, LANES), jnp.float32),
        ),
        in_specs=[vm, vm, pl.BlockSpec(memory_space=pltpu.SMEM)] + [vm] * len(NAMES),
        out_specs=(vm, vm),
        scratch_shapes=[
            pltpu.VMEM((8, pad), jnp.float32),
            pltpu.VMEM((sats, outer, LANES), jnp.float32),
            pltpu.VMEM((sats, outer, 2 * LANES), jnp.float32),
            pltpu.VMEM((dop_rows, 2 * outer, 6 * outer), jnp.bfloat16),
            pltpu.VMEM((dop_rows, 2, outer, LANES), jnp.float32),
            pltpu.VMEM((8, own * LANES), jnp.float32),
        ],
        compiler_params=pltpu.CompilerParams(vmem_limit_bytes=48 * 1024 * 1024),
        name="search",
    )(whole, codes, dopplers, *[jnp.asarray(consts[n]) for n in NAMES])
    detection = lax.pmax(peak[:, 0], "tm")
    return power.reshape(dop_rows, sats, sample_length), detection


def solution(mesh):
    placed = (P(None, "tm", "sat"), P("sat", None), P())
    return jax.shard_map(
        shards,
        mesh=mesh,
        in_specs=placed,
        out_specs=(P("tm", "sat", None), P("sat")),
        check_vma=False,
    )
```

```python
import functools
import math

import jax
import jax.numpy as jnp
import ml_dtypes
import numpy as np
from jax import lax
from jax.experimental import pallas as pl
from jax.experimental.pallas import tpu as pltpu
from jax.sharding import PartitionSpec as P

sample_scale = 2.0 ** (-29)
wrap_count = 32768
LANES = 128
MESH = pl.DeviceIdType.MESH


def halves(table):
    high = table.astype(np.float32).astype(ml_dtypes.bfloat16)
    low = (table - high.astype(np.float64)).astype(np.float32).astype(ml_dtypes.bfloat16)
    return high, low


@functools.lru_cache(maxsize=None)
def tables(sample_length, chip_count):
    inner = LANES
    outer = sample_length // inner
    a = np.arange(outer)
    c = np.arange(inner)
    ang_o = 2 * np.pi * (np.outer(a, a) % outer) / outer
    ang_t = 2 * np.pi * (np.outer(a, c) % sample_length) / sample_length
    ang_i = 2 * np.pi * (np.outer(c, c) % inner) / inner
    fc, fs = np.cos(ang_o), -np.sin(ang_o)
    first = np.block([[fc, -fs], [fs, fc]])
    second = np.block([[-fs, -fc], [fc, -fs]])
    wc, ws = np.cos(ang_i), -np.sin(ang_i)
    fh, fl = halves(np.block([[wc, ws], [-ws, wc]]))
    ih, il = halves(np.block([[wc, -ws], [ws, wc]]))
    bh, bl = halves(np.block([[fc, fs], [-fs, fc]]))
    ch, cl = halves(np.concatenate([fc, fs], axis=0))
    offsets = np.arange(sample_length).reshape(outer, inner)
    chips = offsets * chip_count // sample_length
    signs = 1 - 2 * ((offsets * 2 * chip_count // sample_length) % 2)
    starts = tuple(int(v) for v in chips[:, 0])
    within = chips - chips[:, :1]
    return dict(
        first=first.astype(np.float32),
        second=second.astype(np.float32),
        twist=np.stack([np.cos(ang_t), -np.sin(ang_t)]).astype(np.float32),
        fwd=np.concatenate([fh, fh, fl], axis=0),
        inv=np.concatenate([ih, ih, il], axis=0),
        back=np.concatenate([bh, bh, bl], axis=1),
        code=np.concatenate([ch, cl], axis=1),
        within=within.astype(np.int32),
        signs=signs.astype(np.float32),
    ), starts


NAMES = ("first", "second", "twist", "fwd", "inv", "back", "code", "within", "signs")


def split(value):
    high = value.astype(jnp.bfloat16)
    low = (value - high.astype(jnp.float32)).astype(jnp.bfloat16)
    return high, low


def mm(left, right):
    return jnp.dot(left, right, preferred_element_type=jnp.float32)


def kernel(starts, outer, chip_count, x_ref, codes_ref, dop_ref, *refs):
    count = len(NAMES)
    hbm, refs = refs[:count], refs[count:]
    power_ref, peak_ref = refs[:2]
    tabs, refs = refs[2:2 + count], refs[2 + count:]
    (everyone, cpad, gath, cspec, rot, dtw, energy, acc, peaks, mine,
     tab_sem, own_sem, send1, recv1, send2, recv2, send3, recv3) = refs
    first_ref, second_ref, twist_ref, fwd_ref, inv_ref, back_ref, code_ref, within_ref, signs_ref = tabs
    inner = LANES
    tm_count, sat_count, _, own, rows, _ = everyone.shape
    blocks = tm_count * own
    dop_rows, sats = acc.shape[0], acc.shape[1]
    sample_length = outer * inner
    me_tm, me_sat = lax.axis_index("tm"), lax.axis_index("sat")

    def tm_peer(k):
        return lax.rem(me_tm + k, tm_count)

    def sat_peer(k):
        return lax.rem(me_sat + k, sat_count)

    barrier = pltpu.get_barrier_semaphore()
    for k in range(1, sat_count):
        pl.semaphore_signal(barrier, inc=1, device_id={"sat": sat_peer(k)}, device_id_type=MESH)
    for k in range(1, tm_count):
        pl.semaphore_signal(barrier, inc=1, device_id={"tm": tm_peer(k)}, device_id_type=MESH)

    loads = [pltpu.make_async_copy(h, t, tab_sem.at[i]) for i, (h, t) in enumerate(zip(hbm, tabs))]
    for load in loads:
        load.start()
    place = pltpu.make_async_copy(x_ref, everyone.at[me_tm, me_sat], own_sem)
    place.start()

    cpad[...] = jnp.zeros_like(cpad)
    cpad[0:sats, 0:chip_count] = codes_ref[...].astype(jnp.float32)
    for n1 in range(outer):
        base = starts[n1] // LANES * LANES
        shift = starts[n1] - base
        piece = cpad[:, base:base + 2 * LANES]
        if shift:
            piece = pltpu.roll(piece, 2 * LANES - shift, 1)
        for s in range(sats):
            gath[s, n1:n1 + 1, :] = piece[s:s + 1, :LANES]

    pl.semaphore_wait(barrier, sat_count + tm_count - 2)

    def along_sat(k):
        return pltpu.make_async_remote_copy(
            src_ref=x_ref, dst_ref=everyone.at[me_tm, me_sat], send_sem=send1.at[k - 1],
            recv_sem=recv1.at[k - 1], device_id={"sat": sat_peer(k)}, device_id_type=MESH)

    def from_sat(k):
        src = sat_peer(sat_count - k)
        return pltpu.make_async_remote_copy(
            src_ref=x_ref, dst_ref=everyone.at[me_tm, src], send_sem=send1.at[k - 1],
            recv_sem=recv1.at[k - 1], device_id={"sat": src}, device_id_type=MESH)

    def along_tm(k):
        return pltpu.make_async_remote_copy(
            src_ref=everyone.at[me_tm], dst_ref=everyone.at[me_tm], send_sem=send2.at[k - 1],
            recv_sem=recv2.at[k - 1], device_id={"tm": tm_peer(k)}, device_id_type=MESH)

    def from_tm(k):
        src = tm_peer(tm_count - k)
        return pltpu.make_async_remote_copy(
            src_ref=everyone.at[me_tm], dst_ref=everyone.at[src], send_sem=send2.at[k - 1],
            recv_sem=recv2.at[k - 1], device_id={"tm": src}, device_id_type=MESH)

    def share_peak(k):
        return pltpu.make_async_remote_copy(
            src_ref=mine, dst_ref=peaks.at[k - 1], send_sem=send3.at[k - 1],
            recv_sem=recv3.at[k - 1], device_id={"tm": tm_peer(k)}, device_id_type=MESH)

    for k in range(1, sat_count):
        along_sat(k).start()
    for load in loads:
        load.wait()

    scale = math.sqrt(1.0 / (float(sample_length) ** 3 * blocks))
    t_re, t_im = twist_ref[0], twist_ref[1]
    for s in range(sats):
        rep = jnp.take_along_axis(gath[s], within_ref[...], axis=1) * signs_ref[...]
        rep = rep.astype(jnp.bfloat16)
        y = mm(code_ref[...], jnp.concatenate([rep, rep], axis=0))
        y_re, y_im = y[:outer], y[outer:]
        z = jnp.concatenate([y_re * t_re - y_im * t_im, y_re * t_im + y_im * t_re], axis=1)
        zh, zl = split(z)
        cspec[s] = mm(jnp.concatenate([zh, zl, zh], axis=1), fwd_ref[...]) * scale

    lane = lax.broadcasted_iota(jnp.int32, (8, inner), 1)
    row_of = lax.rem(lane, outer) * inner
    base_row = me_tm * dop_rows
    turn = 2.0 * math.pi / wrap_count
    bins = lax.broadcasted_iota(jnp.int32, (8, inner), 0)
    for f0 in range(0, dop_rows, 4):
        d = jnp.zeros((8, inner), jnp.int32)
        for f in range(f0, min(f0 + 4, dop_rows)):
            d = jnp.where(lax.rem(bins, 4) == f - f0, dop_ref[base_row + f], d)
        m = (jnp.where(bins < 4, row_of, lane) * d) & (wrap_count - 1)
        angle = m.astype(jnp.float32) * turn
        cosine, sine = jnp.cos(angle), -jnp.sin(angle)
        for f in range(f0, min(f0 + 4, dop_rows)):
            i = f - f0
            c1, s1 = cosine[i:i + 1], sine[i:i + 1]
            c2, s2 = cosine[i + 4:i + 5], sine[i + 4:i + 5]
            mh, ml = split(first_ref[...] * c1 + second_ref[...] * s1)
            rot[f] = jnp.concatenate([mh, mh, ml], axis=1)
            dtw[f, 0] = t_re * c2 - t_im * s2
            dtw[f, 1] = t_re * s2 + t_im * c2

    energy[...] = jnp.zeros_like(energy)
    acc[...] = jnp.zeros_like(acc)
    place.wait()
    for k in range(1, sat_count):
        from_sat(k).wait_recv()
    for k in range(1, tm_count):
        along_tm(k).start()

    def group(j, carry):
        @pl.when(j > 0)
        def _():
            from_tm(j).wait_recv()

        g = tm_peer(tm_count - j)
        cols = []
        for blk in range(own):
            parts = [everyone[g, q, part, blk] for part in range(2) for q in range(sat_count)]
            cols.append(jnp.concatenate(parts, axis=0))
        x = jnp.concatenate(cols, axis=1).astype(jnp.float32) * sample_scale
        sq = x * x
        energy[...] += jnp.sum(sq.reshape(2 * outer // 8, 8, own * inner), axis=0)
        xh, xl = split(x)
        xs = jnp.concatenate([xh, xl, xh], axis=0)
        for f in range(dop_rows):
            y = mm(rot[f], xs)
            u_re, u_im = dtw[f, 0], dtw[f, 1]
            zs = []
            for blk in range(own):
                y_re = y[:outer, blk * inner:(blk + 1) * inner]
                y_im = y[outer:, blk * inner:(blk + 1) * inner]
                zs.append(jnp.concatenate([y_re * u_re - y_im * u_im, y_re * u_im + y_im * u_re], axis=1))
            zh, zl = split(jnp.concatenate(zs, axis=0))
            spec = mm(jnp.concatenate([zh, zl, zh], axis=1), fwd_ref[...])
            crosses = []
            for s in range(sats):
                k_re, k_im = cspec[s, :, :inner], cspec[s, :, inner:]
                for blk in range(own):
                    s_re = spec[blk * outer:(blk + 1) * outer, :inner]
                    s_im = spec[blk * outer:(blk + 1) * outer, inner:]
                    crosses.append(jnp.concatenate(
                        [s_re * k_re + s_im * k_im, s_im * k_re - s_re * k_im], axis=1))
            ch, cl = split(jnp.concatenate(crosses, axis=0))
            lag = mm(jnp.concatenate([ch, cl, ch], axis=1), inv_ref[...])
            for s in range(sats):
                cols = []
                for blk in range(own):
                    at = (s * own + blk) * outer
                    l_re, l_im = lag[at:at + outer, :inner], lag[at:at + outer, inner:]
                    cols.append(jnp.concatenate(
                        [l_re * t_re + l_im * t_im, l_im * t_re - l_re * t_im], axis=0))
                wh, wl = split(jnp.concatenate(cols, axis=1))
                out = mm(back_ref[...], jnp.concatenate([wh, wl, wh], axis=0))
                o_re, o_im = out[:outer], out[outer:]
                p = o_re * o_re + o_im * o_im
                total = p[:, :inner]
                for blk in range(1, own):
                    total = total + p[:, blk * inner:(blk + 1) * inner]
                acc[f, s] += total
        return carry

    lax.fori_loop(0, tm_count, group, 0)

    mine[...] = jnp.zeros_like(mine)
    for s in range(sats):
        top = acc[0, s]
        for f in range(1, dop_rows):
            top = jnp.maximum(top, acc[f, s])
        mine[s:s + 1, :] = jnp.max(top, axis=0, keepdims=True)
    for k in range(1, sat_count):
        along_sat(k).wait_send()
    for k in range(1, tm_count):
        along_tm(k).wait_send()
    for f in range(dop_rows):
        for s in range(sats):
            power_ref[s, :, f, :] = acc[f, s]
    for k in range(1, tm_count):
        share_peak(k).start()
    mean = jnp.sum(energy[...]) * (1.0 / float(blocks * sample_length))
    floor = jnp.maximum(mean, 0.25)
    for k in range(1, tm_count):
        share_peak(k).wait()
    best = mine[...]
    for k in range(1, tm_count):
        best = jnp.maximum(best, peaks[k - 1])
    best = jnp.max(best, axis=1, keepdims=True)
    peak_ref[...] = jnp.broadcast_to(best / floor, peak_ref.shape)


def shards(samples, codes, dopplers):
    tm_count, sat_count = lax.axis_size("tm"), lax.axis_size("sat")
    own, segment = samples.shape[1], samples.shape[2]
    sample_length = segment * sat_count
    outer, rows = sample_length // LANES, segment // LANES
    sats, chip_count = codes.shape
    dop_rows = dopplers.shape[0] // tm_count
    consts, starts = tables(sample_length, chip_count)
    local = samples.reshape(2, own, rows, LANES)
    pad = (max(starts) // LANES + 2) * LANES
    pad = max(pad, -(-chip_count // LANES) * LANES)
    peak_rows = -(-sats // 8) * 8
    vm = pl.BlockSpec(memory_space=pltpu.VMEM)
    values = [jnp.asarray(consts[n]) for n in NAMES]
    dma = pltpu.SemaphoreType.DMA
    power, peak = pl.pallas_call(
        functools.partial(kernel, starts, outer, chip_count),
        out_shape=(
            jax.ShapeDtypeStruct((sats, outer, dop_rows, LANES), jnp.float32),
            jax.ShapeDtypeStruct((peak_rows, LANES), jnp.float32),
        ),
        in_specs=[vm, vm, pl.BlockSpec(memory_space=pltpu.SMEM)]
        + [pl.BlockSpec(memory_space=pltpu.HBM)] * len(NAMES),
        out_specs=(vm, vm),
        scratch_shapes=[pltpu.VMEM(v.shape, v.dtype) for v in values] + [
            pltpu.VMEM((tm_count, sat_count) + local.shape, jnp.int32),
            pltpu.VMEM((8, pad), jnp.float32),
            pltpu.VMEM((sats, outer, LANES), jnp.float32),
            pltpu.VMEM((sats, outer, 2 * LANES), jnp.float32),
            pltpu.VMEM((dop_rows, 2 * outer, 6 * outer), jnp.bfloat16),
            pltpu.VMEM((dop_rows, 2, outer, LANES), jnp.float32),
            pltpu.VMEM((8, own * LANES), jnp.float32),
            pltpu.VMEM((dop_rows, sats, outer, LANES), jnp.float32),
            pltpu.VMEM((tm_count - 1, peak_rows, LANES), jnp.float32),
            pltpu.VMEM((peak_rows, LANES), jnp.float32),
            dma((len(NAMES),)),
            dma,
            dma((sat_count - 1,)),
            dma((sat_count - 1,)),
            dma((tm_count - 1,)),
            dma((tm_count - 1,)),
            dma((tm_count - 1,)),
            dma((tm_count - 1,)),
        ],
        compiler_params=pltpu.CompilerParams(
            vmem_limit_bytes=66_500_000, collective_id=0, has_side_effects=True),
        name="search",
    )(local, codes, dopplers, *values)
    power = power.transpose(2, 0, 1, 3).reshape(dop_rows, sats, sample_length)
    return power, peak[:sats, 0]


def solution(mesh):
    placed = (P(None, "tm", "sat"), P("sat", None), P())
    return jax.shard_map(
        shards,
        mesh=mesh,
        in_specs=placed,
        out_specs=(P("tm", "sat", None), P("sat")),
        check_vma=False,
    )
```

```python
import functools
import math

import jax
import jax.numpy as jnp
import ml_dtypes
import numpy as np
from jax import lax
from jax.experimental import pallas as pl
from jax.experimental.pallas import tpu as pltpu
from jax.sharding import PartitionSpec as P

sample_scale = 2.0 ** (-29)
wrap_count = 32768
LANES = 128
KERNEL_BYTES = 65_900_000
PADDING = 1_200_000
MESH = pl.DeviceIdType.MESH


def halves(table):
    high = table.astype(np.float32).astype(ml_dtypes.bfloat16)
    low = (table - high.astype(np.float64)).astype(np.float32).astype(ml_dtypes.bfloat16)
    return high, low


@functools.lru_cache(maxsize=None)
def tables(sample_length, chip_count):
    inner = LANES
    outer = sample_length // inner
    a = np.arange(outer)
    c = np.arange(inner)
    ang_o = 2 * np.pi * (np.outer(a, a) % outer) / outer
    ang_t = 2 * np.pi * (np.outer(a, c) % sample_length) / sample_length
    ang_i = 2 * np.pi * (np.outer(c, c) % inner) / inner
    fc, fs = np.cos(ang_o), -np.sin(ang_o)
    first = np.block([[fc, -fs], [fs, fc]])
    second = np.block([[-fs, -fc], [fc, -fs]])
    wc, ws = np.cos(ang_i), -np.sin(ang_i)
    fh, fl = halves(np.block([[wc, ws], [-ws, wc]]))
    ih, il = halves(np.block([[wc, -ws], [ws, wc]]))
    bh, bl = halves(np.block([[fc, fs], [-fs, fc]]))
    ch, cl = halves(np.concatenate([fc, fs], axis=0))
    offsets = np.arange(sample_length).reshape(outer, inner)
    chips = offsets * chip_count // sample_length
    signs = 1 - 2 * ((offsets * 2 * chip_count // sample_length) % 2)
    starts = tuple(int(v) for v in chips[:, 0])
    within = chips - chips[:, :1]
    wide = np.concatenate([fh, fh, fl, ih, ih, il], axis=0)
    narrow = [first, second, np.cos(ang_t), -np.sin(ang_t), bh, bl,
              np.concatenate([ch, cl], axis=1), within, signs]
    narrow = np.concatenate([np.asarray(t, np.float32) for t in narrow], axis=0)
    return wide, narrow, starts


def padded(table, size):
    extra = -(-size // (table.shape[1] * table.dtype.itemsize)) - table.shape[0]
    return np.pad(table, ((0, max(extra, 0)), (0, 0)))


def split(value):
    high = value.astype(jnp.bfloat16)
    low = (value - high.astype(jnp.float32)).astype(jnp.bfloat16)
    return high, low


def mm(left, right):
    return jnp.dot(left, right, preferred_element_type=jnp.float32)


def kernel(starts, outer, chip_count, cores, x_ref, codes_ref, dop_ref, wide_hbm, narrow_hbm,
           power_ref, peak_ref, raw, chips, wide, narrow, back,
           everyone, cpad, gath, cspec, rot, dtw, energy, acc, peaks, mine,
           tab_sem, send1, recv1, send2, recv2, send3, recv3, send4, recv4):
    inner = LANES
    tm_count, _, line, _, own, rows, _ = everyone.shape
    sat_count = cores * line
    blocks = tm_count * own
    dop_rows, sats = acc.shape[0], acc.shape[1]
    sample_length = outer * inner
    me_tm, me_sat = lax.axis_index("tm"), lax.axis_index("sat")
    me_z, me_core = me_sat // cores, lax.rem(me_sat, cores)
    twin = me_z * cores + (cores - 1 - me_core)

    def tm_peer(k):
        return lax.rem(me_tm + k, tm_count)

    def tm_source(k):
        return lax.rem(me_tm + tm_count - k, tm_count)

    def z_peer(k):
        return lax.rem(me_z + k, line)

    def z_source(k):
        return lax.rem(me_z + line - k, line)

    barrier = pltpu.get_barrier_semaphore()
    for k in range(1, line):
        pl.semaphore_signal(barrier, inc=1, device_id={"sat": z_peer(k) * cores + me_core}, device_id_type=MESH)
    for k in range(1, tm_count):
        pl.semaphore_signal(barrier, inc=1, device_id={"tm": tm_peer(k)}, device_id_type=MESH)
    if cores > 1:
        pl.semaphore_signal(barrier, inc=1, device_id={"sat": twin}, device_id_type=MESH)

    pairs = ((x_ref, raw), (codes_ref, chips),
             (narrow_hbm.at[pl.ds(0, narrow.shape[0])], narrow),
             (wide_hbm.at[pl.ds(0, wide.shape[0])], wide))
    loads = [pltpu.make_async_copy(h, t, tab_sem.at[i]) for i, (h, t) in enumerate(pairs)]
    for load in loads:
        load.start()
    loads[0].wait()
    for part in range(2):
        for r in range(rows):
            piece = raw[part, :, r * LANES:(r + 1) * LANES]
            for blk in range(own):
                everyone[me_tm, me_core, me_z, part, blk, r:r + 1, :] = piece[blk:blk + 1]
    loads[1].wait()

    cpad[...] = jnp.zeros_like(cpad)
    cpad[0:sats, 0:chip_count] = chips[...].astype(jnp.float32)
    for n1 in range(outer):
        base = starts[n1] // LANES * LANES
        shift = starts[n1] - base
        piece = cpad[:, base:base + 2 * LANES]
        if shift:
            piece = pltpu.roll(piece, 2 * LANES - shift, 1)
        for s in range(sats):
            gath[s, n1:n1 + 1, :] = piece[s:s + 1, :LANES]

    pl.semaphore_wait(barrier, line + tm_count + cores - 3)

    def along_z(k, at):
        return pltpu.make_async_remote_copy(
            src_ref=everyone.at[me_tm, me_core, me_z], dst_ref=everyone.at[me_tm, me_core, at],
            send_sem=send1.at[k - 1], recv_sem=recv1.at[k - 1],
            device_id={"sat": z_peer(k) * cores + me_core}, device_id_type=MESH)

    def along_tm(k, at):
        return pltpu.make_async_remote_copy(
            src_ref=everyone.at[me_tm, me_core], dst_ref=everyone.at[at, me_core],
            send_sem=send2.at[k - 1], recv_sem=recv2.at[k - 1],
            device_id={"tm": tm_peer(k)}, device_id_type=MESH)

    def to_twin(k, at_core):
        g = tm_source(k)
        return pltpu.make_async_remote_copy(
            src_ref=everyone.at[g, me_core], dst_ref=everyone.at[g, at_core],
            send_sem=send4.at[k], recv_sem=recv4.at[k],
            device_id={"sat": twin}, device_id_type=MESH)

    def share_peak(k):
        return pltpu.make_async_remote_copy(
            src_ref=mine, dst_ref=peaks.at[k - 1], send_sem=send3.at[k - 1],
            recv_sem=recv3.at[k - 1], device_id={"tm": tm_peer(k)}, device_id_type=MESH)

    for k in range(1, line):
        along_z(k, me_z).start()
    loads[2].wait()
    loads[3].wait()

    cut = [0]

    def take(count):
        cut.append(cut[-1] + count)
        return narrow[cut[-2]:cut[-1]]

    first, second = take(2 * outer), take(2 * outer)
    t_re, t_im = take(outer), take(outer)
    bh, bl = take(2 * outer).astype(jnp.bfloat16), take(2 * outer).astype(jnp.bfloat16)
    back[...] = jnp.concatenate([bh, bh, bl], axis=1)
    code = take(2 * outer).astype(jnp.bfloat16)
    within = take(outer).astype(jnp.int32)
    signs = take(outer)
    t_at = 4 * outer
    fwd_ref = wide.at[pl.ds(0, 6 * inner)]
    inv_ref = wide.at[pl.ds(6 * inner, 6 * inner)]
    scale = math.sqrt(1.0 / (float(sample_length) ** 3 * blocks))
    for s in range(sats):
        rep = jnp.take_along_axis(gath[s], within, axis=1) * signs
        rep = rep.astype(jnp.bfloat16)
        y = mm(code, jnp.concatenate([rep, rep], axis=0))
        y_re, y_im = y[:outer], y[outer:]
        z = jnp.concatenate([y_re * t_re - y_im * t_im, y_re * t_im + y_im * t_re], axis=1)
        zh, zl = split(z)
        cspec[s] = mm(jnp.concatenate([zh, zl, zh], axis=1), fwd_ref[...]) * scale

    lane = lax.broadcasted_iota(jnp.int32, (8, inner), 1)
    row_of = lax.rem(lane, outer) * inner
    base_row = me_tm * dop_rows
    turn = 2.0 * math.pi / wrap_count
    bins = lax.broadcasted_iota(jnp.int32, (8, inner), 0)
    for f0 in range(0, dop_rows, 4):
        d = jnp.zeros((8, inner), jnp.int32)
        for f in range(f0, min(f0 + 4, dop_rows)):
            d = jnp.where(lax.rem(bins, 4) == f - f0, dop_ref[base_row + f], d)
        m = (jnp.where(bins < 4, row_of, lane) * d) & (wrap_count - 1)
        angle = m.astype(jnp.float32) * turn
        cosine, sine = jnp.cos(angle), -jnp.sin(angle)
        for f in range(f0, min(f0 + 4, dop_rows)):
            i = f - f0
            c1, s1 = cosine[i:i + 1], sine[i:i + 1]
            c2, s2 = cosine[i + 4:i + 5], sine[i + 4:i + 5]
            mh, ml = split(first * c1 + second * s1)
            rot[f] = jnp.concatenate([mh, mh, ml], axis=1)
            dtw[f, 0] = t_re * c2 - t_im * s2
            dtw[f, 1] = t_re * s2 + t_im * c2

    energy[...] = jnp.zeros_like(energy)
    acc[...] = jnp.zeros_like(acc)
    for k in range(1, line):
        along_z(k, z_source(k)).wait_recv()
    for k in range(1, tm_count):
        along_tm(k, me_tm).start()
    if cores > 1:
        to_twin(0, me_core).start()

    def group(j, carry):
        @pl.when(j == 1)
        def _():
            along_tm(j, tm_source(j)).wait_recv()
            if cores > 1:
                to_twin(j, me_core).start()

        @pl.when((j > 0) & (j < tm_count - 1))
        def _():
            along_tm(j + 1, tm_source(j + 1)).wait_recv()
            if cores > 1:
                to_twin(j + 1, me_core).start()

        if cores > 1:
            to_twin(j, cores - 1 - me_core).wait_recv()
        g = tm_source(j)
        w_re, w_im = narrow[t_at:t_at + outer], narrow[t_at + outer:t_at + 2 * outer]
        cols = []
        for blk in range(own):
            parts = [everyone[g, q % cores, q // cores, part, blk] for part in range(2) for q in range(sat_count)]
            cols.append(jnp.concatenate(parts, axis=0))
        x = jnp.concatenate(cols, axis=1).astype(jnp.float32) * sample_scale
        sq = x * x
        energy[...] += jnp.sum(sq.reshape(2 * outer // 8, 8, own * inner), axis=0)
        xh, xl = split(x)
        xs = jnp.concatenate([xh, xl, xh], axis=0)
        for f in range(dop_rows):
            y = mm(rot[f], xs)
            u_re, u_im = dtw[f, 0], dtw[f, 1]
            zs = []
            for blk in range(own):
                y_re = y[:outer, blk * inner:(blk + 1) * inner]
                y_im = y[outer:, blk * inner:(blk + 1) * inner]
                zs.append(jnp.concatenate([y_re * u_re - y_im * u_im, y_re * u_im + y_im * u_re], axis=1))
            zh, zl = split(jnp.concatenate(zs, axis=0))
            spec = mm(jnp.concatenate([zh, zl, zh], axis=1), fwd_ref[...])
            crosses = []
            for s in range(sats):
                k_re, k_im = cspec[s, :, :inner], cspec[s, :, inner:]
                for blk in range(own):
                    s_re = spec[blk * outer:(blk + 1) * outer, :inner]
                    s_im = spec[blk * outer:(blk + 1) * outer, inner:]
                    crosses.append(jnp.concatenate(
                        [s_re * k_re + s_im * k_im, s_im * k_re - s_re * k_im], axis=1))
            ch, cl = split(jnp.concatenate(crosses, axis=0))
            lag = mm(jnp.concatenate([ch, cl, ch], axis=1), inv_ref[...])
            for s in range(sats):
                cols = []
                for blk in range(own):
                    at = (s * own + blk) * outer
                    l_re, l_im = lag[at:at + outer, :inner], lag[at:at + outer, inner:]
                    cols.append(jnp.concatenate(
                        [l_re * w_re + l_im * w_im, l_im * w_re - l_re * w_im], axis=0))
                wh, wl = split(jnp.concatenate(cols, axis=1))
                out = mm(back[...], jnp.concatenate([wh, wl, wh], axis=0))
                o_re, o_im = out[:outer], out[outer:]
                p = o_re * o_re + o_im * o_im
                total = p[:, :inner]
                for blk in range(1, own):
                    total = total + p[:, blk * inner:(blk + 1) * inner]
                acc[f, s] += total
        return carry

    lax.fori_loop(0, tm_count, group, 0)

    mine[...] = jnp.zeros_like(mine)
    for s in range(sats):
        top = acc[0, s]
        for f in range(1, dop_rows):
            top = jnp.maximum(top, acc[f, s])
        mine[s:s + 1, :] = jnp.max(top, axis=0, keepdims=True)
    for k in range(1, line):
        along_z(k, me_z).wait_send()
    for k in range(1, tm_count):
        along_tm(k, me_tm).wait_send()
    if cores > 1:
        for k in range(tm_count):
            to_twin(k, me_core).wait_send()
    for f in range(dop_rows):
        for s in range(sats):
            power_ref[s, :, f, :] = acc[f, s]
    for k in range(1, tm_count):
        share_peak(k).start()
    mean = jnp.sum(energy[...]) * (1.0 / float(blocks * sample_length))
    floor = jnp.maximum(mean, 0.25)
    for k in range(1, tm_count):
        share_peak(k).wait()
    best = mine[...]
    for k in range(1, tm_count):
        best = jnp.maximum(best, peaks[k - 1])
    best = jnp.max(best, axis=1, keepdims=True)
    peak_ref[...] = jnp.broadcast_to(best / floor, peak_ref.shape)


def shards(samples, codes, dopplers):
    tm_count, sat_count = lax.axis_size("tm"), lax.axis_size("sat")
    own, segment = samples.shape[1], samples.shape[2]
    sample_length = segment * sat_count
    outer, rows = sample_length // LANES, segment // LANES
    sats, chip_count = codes.shape
    dop_rows = dopplers.shape[0] // tm_count
    cores = 2 if sat_count % 2 == 0 else 1
    line = sat_count // cores
    wide, narrow, starts = tables(sample_length, chip_count)
    pad = (max(starts) // LANES + 2) * LANES
    pad = max(pad, -(-chip_count // LANES) * LANES)
    peak_rows = -(-sats // 8) * 8
    vm = pl.BlockSpec(memory_space=pltpu.VMEM)
    hbm = pl.BlockSpec(memory_space=pltpu.HBM)
    dma = pltpu.SemaphoreType.DMA
    power, peak = pl.pallas_call(
        functools.partial(kernel, starts, outer, chip_count, cores),
        out_shape=(
            jax.ShapeDtypeStruct((sats, outer, dop_rows, LANES), jnp.float32),
            jax.ShapeDtypeStruct((peak_rows, LANES), jnp.float32),
        ),
        in_specs=[hbm, hbm, pl.BlockSpec(memory_space=pltpu.SMEM), hbm, hbm],
        out_specs=(vm, vm),
        scratch_shapes=[
            pltpu.VMEM(samples.shape, jnp.int32),
            pltpu.VMEM(codes.shape, jnp.int32),
            pltpu.VMEM(wide.shape, jnp.bfloat16),
            pltpu.VMEM(narrow.shape, jnp.float32),
            pltpu.VMEM((2 * outer, 6 * outer), jnp.bfloat16),
            pltpu.VMEM((tm_count, cores, line, 2, own, rows, LANES), jnp.int32),
            pltpu.VMEM((8, pad), jnp.float32),
            pltpu.VMEM((sats, outer, LANES), jnp.float32),
            pltpu.VMEM((sats, outer, 2 * LANES), jnp.float32),
            pltpu.VMEM((dop_rows, 2 * outer, 6 * outer), jnp.bfloat16),
            pltpu.VMEM((dop_rows, 2, outer, LANES), jnp.float32),
            pltpu.VMEM((8, own * LANES), jnp.float32),
            pltpu.VMEM((dop_rows, sats, outer, LANES), jnp.float32),
            pltpu.VMEM((tm_count - 1, peak_rows, LANES), jnp.float32),
            pltpu.VMEM((peak_rows, LANES), jnp.float32),
            dma((4,)),
            dma((line - 1,)),
            dma((line - 1,)),
            dma((tm_count - 1,)),
            dma((tm_count - 1,)),
            dma((tm_count - 1,)),
            dma((tm_count - 1,)),
            dma((tm_count,)),
            dma((tm_count,)),
        ],
        compiler_params=pltpu.CompilerParams(
            vmem_limit_bytes=KERNEL_BYTES, collective_id=0, has_side_effects=True),
        name="search",
    )(samples, codes, dopplers, jnp.asarray(padded(wide, PADDING)), jnp.asarray(padded(narrow, PADDING)))
    power = power.transpose(2, 0, 1, 3).reshape(dop_rows, sats, sample_length)
    return power, peak[:sats, 0]


def solution(mesh):
    placed = (P(None, "tm", "sat"), P("sat", None), P())
    return jax.shard_map(
        shards,
        mesh=mesh,
        in_specs=placed,
        out_specs=(P("tm", "sat", None), P("sat")),
        check_vma=False,
    )
```

```python
import functools
import math

import jax
import jax.numpy as jnp
import ml_dtypes
import numpy as np
from jax import lax
from jax.experimental import pallas as pl
from jax.experimental.pallas import tpu as pltpu
from jax.sharding import PartitionSpec as P

sample_scale = 2.0 ** (-29)
wrap_count = 32768
LANES = 128
KERNEL_BYTES = 55_800_000
PADDING = 1_200_000
MESH = pl.DeviceIdType.MESH


def halves(table):
    high = table.astype(np.float32).astype(ml_dtypes.bfloat16)
    low = (table - high.astype(np.float64)).astype(np.float32).astype(ml_dtypes.bfloat16)
    return high, low


@functools.lru_cache(maxsize=None)
def tables(sample_length, chip_count):
    inner = LANES
    outer = sample_length // inner
    a = np.arange(outer)
    c = np.arange(inner)
    ang_o = 2 * np.pi * (np.outer(a, a) % outer) / outer
    ang_t = 2 * np.pi * (np.outer(a, c) % sample_length) / sample_length
    ang_i = 2 * np.pi * (np.outer(c, c) % inner) / inner
    fc, fs = np.cos(ang_o), -np.sin(ang_o)
    first = np.block([[fc, -fs], [fs, fc]])
    second = np.block([[-fs, -fc], [fc, -fs]])
    wc, ws = np.cos(ang_i), -np.sin(ang_i)
    fh, fl = halves(np.block([[wc, ws], [-ws, wc]]))
    ih, il = halves(np.block([[wc, -ws], [ws, wc]]))
    bh, bl = halves(np.block([[fc, fs], [-fs, fc]]))
    ch, cl = halves(np.concatenate([fc, fs], axis=0))
    offsets = np.arange(sample_length).reshape(outer, inner)
    chips = offsets * chip_count // sample_length
    signs = 1 - 2 * ((offsets * 2 * chip_count // sample_length) % 2)
    starts = tuple(int(v) for v in chips[:, 0])
    within = chips - chips[:, :1]
    wide = np.concatenate([fh, fh, fl, ih, ih, il], axis=0)
    narrow = [first, second, np.cos(ang_t), -np.sin(ang_t), bh, bl,
              np.concatenate([ch, cl], axis=1), within, signs]
    narrow = np.concatenate([np.asarray(t, np.float32) for t in narrow], axis=0)
    return wide, narrow, starts


def padded(table, size):
    extra = -(-size // (table.shape[1] * table.dtype.itemsize)) - table.shape[0]
    return np.pad(table, ((0, max(extra, 0)), (0, 0)))


def split(value):
    high = value.astype(jnp.bfloat16)
    low = (value - high.astype(jnp.float32)).astype(jnp.bfloat16)
    return high, low


def mm(left, right):
    return jnp.dot(left, right, preferred_element_type=jnp.float32)


def kernel(starts, outer, chip_count, cores, x_ref, codes_ref, dop_ref, wide_hbm, narrow_hbm,
           power_ref, peak_ref, raw, chips, wide, narrow, back,
           everyone, cpad, gath, cspec, rot, dtw, energy, acc, peaks, mine,
           tab_sem, send1, recv1, send2, recv2, send3, recv3, send4, recv4):
    inner = LANES
    tm_count, _, line, _, own, rows, _ = everyone.shape
    sat_count = cores * line
    blocks = tm_count * own
    dop_rows, sats = acc.shape[0], acc.shape[1]
    sample_length = outer * inner
    me_tm, me_sat = lax.axis_index("tm"), lax.axis_index("sat")
    me_z, me_core = me_sat // cores, lax.rem(me_sat, cores)
    twin = me_z * cores + (cores - 1 - me_core)

    paired = tm_count & (tm_count - 1) == 0

    def tm_peer(k):
        if not paired:
            return lax.rem(me_tm + k, tm_count)
        peer, bit = 0, 1
        while bit < tm_count:
            peer = peer + ((me_tm // bit + k // bit) % 2) * bit
            bit *= 2
        return peer

    def tm_source(k):
        return tm_peer(k) if paired else lax.rem(me_tm + tm_count - k, tm_count)

    def z_peer(k):
        return lax.rem(me_z + k, line)

    def z_source(k):
        return lax.rem(me_z + line - k, line)

    barrier = pltpu.get_barrier_semaphore()
    for k in range(1, line):
        pl.semaphore_signal(barrier, inc=1, device_id={"sat": z_peer(k) * cores + me_core}, device_id_type=MESH)
    for k in range(1, tm_count):
        pl.semaphore_signal(barrier, inc=1, device_id={"tm": tm_peer(k)}, device_id_type=MESH)
    if cores > 1:
        pl.semaphore_signal(barrier, inc=1, device_id={"sat": twin}, device_id_type=MESH)

    pairs = ((x_ref, raw), (codes_ref, chips),
             (narrow_hbm.at[pl.ds(0, narrow.shape[0])], narrow),
             (wide_hbm.at[pl.ds(0, wide.shape[0])], wide))
    loads = [pltpu.make_async_copy(h, t, tab_sem.at[i]) for i, (h, t) in enumerate(pairs)]
    for load in loads:
        load.start()
    loads[0].wait()
    for part in range(2):
        for r in range(rows):
            piece = raw[part, :, r * LANES:(r + 1) * LANES]
            for blk in range(own):
                everyone[me_tm, me_core, me_z, part, blk, r:r + 1, :] = piece[blk:blk + 1]
    loads[1].wait()

    cpad[...] = jnp.zeros_like(cpad)
    cpad[0:sats, 0:chip_count] = chips[...].astype(jnp.float32)
    for n1 in range(outer):
        base = starts[n1] // LANES * LANES
        shift = starts[n1] - base
        piece = cpad[:, base:base + 2 * LANES]
        if shift:
            piece = pltpu.roll(piece, 2 * LANES - shift, 1)
        for s in range(sats):
            gath[s, n1:n1 + 1, :] = piece[s:s + 1, :LANES]

    pl.semaphore_wait(barrier, line + tm_count + cores - 3)

    def along_z(k, at):
        return pltpu.make_async_remote_copy(
            src_ref=everyone.at[me_tm, me_core, me_z], dst_ref=everyone.at[me_tm, me_core, at],
            send_sem=send1.at[k - 1], recv_sem=recv1.at[k - 1],
            device_id={"sat": z_peer(k) * cores + me_core}, device_id_type=MESH)

    def along_tm(k, at):
        return pltpu.make_async_remote_copy(
            src_ref=everyone.at[me_tm, me_core], dst_ref=everyone.at[at, me_core],
            send_sem=send2.at[k - 1], recv_sem=recv2.at[k - 1],
            device_id={"tm": tm_peer(k)}, device_id_type=MESH)

    def to_twin(k, at_core):
        g = tm_source(k)
        return pltpu.make_async_remote_copy(
            src_ref=everyone.at[g, me_core], dst_ref=everyone.at[g, at_core],
            send_sem=send4.at[k], recv_sem=recv4.at[k],
            device_id={"sat": twin}, device_id_type=MESH)

    def share_peak(k):
        return pltpu.make_async_remote_copy(
            src_ref=mine, dst_ref=peaks.at[k - 1], send_sem=send3.at[k - 1],
            recv_sem=recv3.at[k - 1], device_id={"tm": tm_peer(k)}, device_id_type=MESH)

    for k in range(1, line):
        along_z(k, me_z).start()
    loads[2].wait()
    loads[3].wait()

    cut = [0]

    def take(count):
        cut.append(cut[-1] + count)
        return narrow[cut[-2]:cut[-1]]

    first, second = take(2 * outer), take(2 * outer)
    t_re, t_im = take(outer), take(outer)
    bh, bl = take(2 * outer).astype(jnp.bfloat16), take(2 * outer).astype(jnp.bfloat16)
    back[...] = jnp.concatenate([bh, bh, bl], axis=1)
    code = take(2 * outer).astype(jnp.bfloat16)
    within = take(outer).astype(jnp.int32)
    signs = take(outer)
    t_at = 4 * outer
    fwd_ref = wide.at[pl.ds(0, 6 * inner)]
    inv_ref = wide.at[pl.ds(6 * inner, 6 * inner)]
    scale = math.sqrt(1.0 / (float(sample_length) ** 3 * blocks))
    for s in range(sats):
        rep = jnp.take_along_axis(gath[s], within, axis=1) * signs
        rep = rep.astype(jnp.bfloat16)
        y = mm(code, jnp.concatenate([rep, rep], axis=0))
        y_re, y_im = y[:outer], y[outer:]
        z = jnp.concatenate([y_re * t_re - y_im * t_im, y_re * t_im + y_im * t_re], axis=1)
        zh, zl = split(z)
        cspec[s] = mm(jnp.concatenate([zh, zl, zh], axis=1), fwd_ref[...]) * scale

    lane = lax.broadcasted_iota(jnp.int32, (8, inner), 1)
    row_of = lax.rem(lane, outer) * inner
    base_row = me_tm * dop_rows
    turn = 2.0 * math.pi / wrap_count
    bins = lax.broadcasted_iota(jnp.int32, (8, inner), 0)
    for f0 in range(0, dop_rows, 4):
        d = jnp.zeros((8, inner), jnp.int32)
        for f in range(f0, min(f0 + 4, dop_rows)):
            d = jnp.where(lax.rem(bins, 4) == f - f0, dop_ref[base_row + f], d)
        m = (jnp.where(bins < 4, row_of, lane) * d) & (wrap_count - 1)
        angle = m.astype(jnp.float32) * turn
        cosine, sine = jnp.cos(angle), -jnp.sin(angle)
        for f in range(f0, min(f0 + 4, dop_rows)):
            i = f - f0
            c1, s1 = cosine[i:i + 1], sine[i:i + 1]
            c2, s2 = cosine[i + 4:i + 5], sine[i + 4:i + 5]
            mh, ml = split(first * c1 + second * s1)
            rot[f] = jnp.concatenate([mh, mh, ml], axis=1)
            dtw[f, 0] = t_re * c2 - t_im * s2
            dtw[f, 1] = t_re * s2 + t_im * c2

    energy[...] = jnp.zeros_like(energy)
    acc[...] = jnp.zeros_like(acc)
    for k in range(1, line):
        along_z(k, z_source(k)).wait_recv()
    for k in range(1, tm_count):
        along_tm(k, me_tm).start()
    if cores > 1:
        to_twin(0, me_core).start()

    def group(j, carry):
        @pl.when(j == 1)
        def _():
            along_tm(j, tm_source(j)).wait_recv()
            if cores > 1:
                to_twin(j, me_core).start()

        @pl.when((j > 0) & (j < tm_count - 1))
        def _():
            along_tm(j + 1, tm_source(j + 1)).wait_recv()
            if cores > 1:
                to_twin(j + 1, me_core).start()

        if cores > 1:
            to_twin(j, cores - 1 - me_core).wait_recv()
        g = tm_source(j)
        w_re, w_im = narrow[t_at:t_at + outer], narrow[t_at + outer:t_at + 2 * outer]
        cols = []
        for blk in range(own):
            parts = [everyone[g, q % cores, q // cores, part, blk] for part in range(2) for q in range(sat_count)]
            cols.append(jnp.concatenate(parts, axis=0))
        x = jnp.concatenate(cols, axis=1).astype(jnp.float32) * sample_scale
        sq = x * x
        energy[...] += jnp.sum(sq.reshape(2 * outer // 8, 8, own * inner), axis=0)
        xh, xl = split(x)
        xs = jnp.concatenate([xh, xl, xh], axis=0)
        for f in range(dop_rows):
            y = mm(rot[f], xs)
            u_re, u_im = dtw[f, 0], dtw[f, 1]
            zs = []
            for blk in range(own):
                y_re = y[:outer, blk * inner:(blk + 1) * inner]
                y_im = y[outer:, blk * inner:(blk + 1) * inner]
                zs.append(jnp.concatenate([y_re * u_re - y_im * u_im, y_re * u_im + y_im * u_re], axis=1))
            zh, zl = split(jnp.concatenate(zs, axis=0))
            spec = mm(jnp.concatenate([zh, zl, zh], axis=1), fwd_ref[...])
            crosses = []
            for s in range(sats):
                k_re, k_im = cspec[s, :, :inner], cspec[s, :, inner:]
                for blk in range(own):
                    s_re = spec[blk * outer:(blk + 1) * outer, :inner]
                    s_im = spec[blk * outer:(blk + 1) * outer, inner:]
                    crosses.append(jnp.concatenate(
                        [s_re * k_re + s_im * k_im, s_im * k_re - s_re * k_im], axis=1))
            ch, cl = split(jnp.concatenate(crosses, axis=0))
            lag = mm(jnp.concatenate([ch, cl, ch], axis=1), inv_ref[...])
            for s in range(sats):
                cols = []
                for blk in range(own):
                    at = (s * own + blk) * outer
                    l_re, l_im = lag[at:at + outer, :inner], lag[at:at + outer, inner:]
                    cols.append(jnp.concatenate(
                        [l_re * w_re + l_im * w_im, l_im * w_re - l_re * w_im], axis=0))
                wh, wl = split(jnp.concatenate(cols, axis=1))
                out = mm(back[...], jnp.concatenate([wh, wl, wh], axis=0))
                o_re, o_im = out[:outer], out[outer:]
                p = o_re * o_re + o_im * o_im
                total = p[:, :inner]
                for blk in range(1, own):
                    total = total + p[:, blk * inner:(blk + 1) * inner]
                acc[f, s] += total
        return carry

    lax.fori_loop(0, tm_count, group, 0)

    mine[...] = jnp.zeros_like(mine)
    for s in range(sats):
        top = acc[0, s]
        for f in range(1, dop_rows):
            top = jnp.maximum(top, acc[f, s])
        mine[s:s + 1, :] = jnp.max(top, axis=0, keepdims=True)
    for k in range(1, line):
        along_z(k, me_z).wait_send()
    for k in range(1, tm_count):
        along_tm(k, me_tm).wait_send()
    if cores > 1:
        for k in range(tm_count):
            to_twin(k, me_core).wait_send()
    for f in range(dop_rows):
        for s in range(sats):
            power_ref[s, :, f, :] = acc[f, s]
    for k in range(1, tm_count):
        share_peak(k).start()
    mean = jnp.sum(energy[...]) * (1.0 / float(blocks * sample_length))
    floor = jnp.maximum(mean, 0.25)
    for k in range(1, tm_count):
        share_peak(k).wait()
    best = mine[...]
    for k in range(1, tm_count):
        best = jnp.maximum(best, peaks[k - 1])
    best = jnp.max(best, axis=1, keepdims=True)
    peak_ref[...] = jnp.broadcast_to(best / floor, peak_ref.shape)


def shards(samples, codes, dopplers):
    tm_count, sat_count = lax.axis_size("tm"), lax.axis_size("sat")
    own, segment = samples.shape[1], samples.shape[2]
    sample_length = segment * sat_count
    outer, rows = sample_length // LANES, segment // LANES
    sats, chip_count = codes.shape
    dop_rows = dopplers.shape[0] // tm_count
    cores = 2 if sat_count % 2 == 0 else 1
    line = sat_count // cores
    wide, narrow, starts = tables(sample_length, chip_count)
    pad = (max(starts) // LANES + 2) * LANES
    pad = max(pad, -(-chip_count // LANES) * LANES)
    peak_rows = -(-sats // 8) * 8
    vm = pl.BlockSpec(memory_space=pltpu.VMEM)
    hbm = pl.BlockSpec(memory_space=pltpu.HBM)
    dma = pltpu.SemaphoreType.DMA
    power, peak = pl.pallas_call(
        functools.partial(kernel, starts, outer, chip_count, cores),
        out_shape=(
            jax.ShapeDtypeStruct((sats, outer, dop_rows, LANES), jnp.float32),
            jax.ShapeDtypeStruct((peak_rows, LANES), jnp.float32),
        ),
        in_specs=[hbm, hbm, pl.BlockSpec(memory_space=pltpu.SMEM), hbm, hbm],
        out_specs=(vm, vm),
        scratch_shapes=[
            pltpu.VMEM(samples.shape, jnp.int32),
            pltpu.VMEM(codes.shape, jnp.int32),
            pltpu.VMEM(wide.shape, jnp.bfloat16),
            pltpu.VMEM(narrow.shape, jnp.float32),
            pltpu.VMEM((2 * outer, 6 * outer), jnp.bfloat16),
            pltpu.VMEM((tm_count, cores, line, 2, own, rows, LANES), jnp.int32),
            pltpu.VMEM((8, pad), jnp.float32),
            pltpu.VMEM((sats, outer, LANES), jnp.float32),
            pltpu.VMEM((sats, outer, 2 * LANES), jnp.float32),
            pltpu.VMEM((dop_rows, 2 * outer, 6 * outer), jnp.bfloat16),
            pltpu.VMEM((dop_rows, 2, outer, LANES), jnp.float32),
            pltpu.VMEM((8, own * LANES), jnp.float32),
            pltpu.VMEM((dop_rows, sats, outer, LANES), jnp.float32),
            pltpu.VMEM((tm_count - 1, peak_rows, LANES), jnp.float32),
            pltpu.VMEM((peak_rows, LANES), jnp.float32),
            dma((4,)),
            dma((line - 1,)),
            dma((line - 1,)),
            dma((tm_count - 1,)),
            dma((tm_count - 1,)),
            dma((tm_count - 1,)),
            dma((tm_count - 1,)),
            dma((tm_count,)),
            dma((tm_count,)),
        ],
        compiler_params=pltpu.CompilerParams(
            vmem_limit_bytes=KERNEL_BYTES, collective_id=0, has_side_effects=True),
        name="search",
    )(samples, codes, dopplers, jnp.asarray(padded(wide, PADDING)), jnp.asarray(padded(narrow, PADDING)))
    power = power.transpose(2, 0, 1, 3).reshape(dop_rows, sats, sample_length)
    return power, peak[:sats, 0]


def solution(mesh):
    placed = (P(None, "tm", "sat"), P("sat", None), P())
    return jax.shard_map(
        shards,
        mesh=mesh,
        in_specs=placed,
        out_specs=(P("tm", "sat", None), P("sat")),
        check_vma=False,
    )
```
